32 devices in a mesh: row: 8 (over y, x, core), col: 4 (over z).
Axes of the slice: x: 2, y: 2, z: 4, core: 2. Of those that a mesh axis runs over, the one named last changes fastest.
Arguments:
- grad_out: bfloat16 [256, 128, 320], P('row', 'col'), may hold values from -0.078125 to 0.078125
- dec_pre: bfloat16 [256, 128, 320], P('row', 'col'), may hold values from -6 to 6
- ctrl_out: bfloat16 [256, 128, 320], P('row', 'col'), may hold values from -6 to 6
- ctrl_mid: bfloat16 [256, 128, 320], P('row', 'col'), may hold values from -6 to 6
- ctrl_in: bfloat16 [256, 128, 320], P('row', 'col'), may hold values from -6 to 6
- dec_weight: bfloat16 [3, 3, 320, 320], replicated, may hold values from -0.109375 to 0.109375
- zero_weight: bfloat16 [320, 320], replicated, may hold values from -0.3125 to 0.3125
- ctrl_weight: bfloat16 [3, 3, 320, 320], replicated, may hold values from -0.109375 to 0.109375
Outputs:
- grad_zero: float32 [320, 320], P('row', 'col')
- grad_ctrl: float32 [3, 3, 320, 320], P(None, None, 'row', 'col')
- grad_in: float32 [3, 3, 320, 320], P(None, None, 'row', 'col')
The draws below stay inside these ranges and needn't reach their ends.
All inputs are finite; a program needn't handle non-finite values.
Results may differ from the reference program's by a relative error of at most 0.024.
Values may be sent and summed in bfloat16 or wider, within the bound.
No kernel may reach another device: no remote copies, remote signals or barrier semaphores. Data moves between devices by JAX's collectives and lax.ppermute only.
A program may use at most 128 MiB of HBM per device.

```python
import jax
import jax.numpy as jnp
from jax import lax

C = 320
TH = 32
NH = 256
NW = 128
N_ROW = 8


def raised(values, rng, source, target, shards_of, factor):
    def block_of(position):
        return (jnp.arange(values.shape[position]) // (values.shape[position] // shards_of)).reshape((-1,) + (1,) * (values.ndim - 1 - position))

    near = jax.random.permutation(rng, shards_of)[block_of(target)]
    other_side = (block_of(target) + shards_of // 2) % shards_of
    return jnp.where((block_of(source) == near) | (block_of(source) == other_side), factor * values, values)


def block_scale(key, dims, split, least, largest):
    level = 1.0
    for dim, parts in split:
        heights = jax.random.uniform(jax.random.fold_in(jax.random.fold_in(key, 6), dim), (parts,), jnp.float32, least / len(split), largest / len(split))
        level = level * jnp.repeat(jnp.exp(heights), dims[dim] // parts).reshape((-1,) + (1,) * (len(dims) - 1 - dim))
    return level


def centred(rng, dims, scale, most, pieces=(), kind=jnp.bfloat16):
    gain = block_scale(rng, dims, pieces, -0.22, 0.18) if pieces else 1.0
    entries = jax.random.normal(rng, dims, jnp.float32) * scale * gain
    return jnp.minimum(jnp.maximum(entries, -most), most).astype(kind)


def bell_draw_with(own_key, extent, width, reach, pieces, heavy, kind=jnp.bfloat16):
    entries = width * jax.random.normal(own_key, extent, jnp.float32)
    if pieces:
        entries = entries * block_scale(own_key, extent, pieces, -0.22, 0.18)
    return jnp.clip(raised(entries, jax.random.fold_in(own_key, 3), *heavy), -reach, reach).astype(kind)


def setup_inputs(seed: int = 0) -> dict:
    key_of = jax.random.split(jax.random.key(seed), 9)
    grad_out = bell_draw_with(key_of[0], (NH, NW, C), (1.0 / (TH * N_ROW)), 0.078125, ((0, 8), (1, 4)), (0, 2, 8, 2.0))
    dec_pre = centred(key_of[1], (NH, NW, C), 1.0, 6.0, ((0, 8), (1, 4)))
    ctrl_out = bell_draw_with(key_of[2], (NH, NW, C), 1.0, 6.0, ((0, 8), (1, 4)), (1, 2, 4, 2.0))
    ctrl_mid = centred(key_of[3], (NH, NW, C), 1.0, 6.0, ((0, 8), (1, 4)))
    ctrl_in = bell_draw_with(key_of[4], (NH, NW, C), 1.0, 6.0, ((0, 8), (1, 4)), (0, 2, 8, 2.0))
    dec_weight = centred(key_of[5], (3, 3, C, C), (9 * C) ** -0.5, 0.109375)
    zero_weight = centred(key_of[6], (C, C), C ** -0.5, 0.3125)
    ctrl_weight = centred(key_of[7], (3, 3, C, C), (9 * C) ** -0.5, 0.109375)
    return dict(grad_out=grad_out, dec_pre=dec_pre, ctrl_out=ctrl_out, ctrl_mid=ctrl_mid, ctrl_in=ctrl_in, dec_weight=dec_weight, zero_weight=zero_weight, ctrl_weight=ctrl_weight)


def silu_slope(values):
    sigm = jax.nn.sigmoid(values)
    return sigm * (1.0 + values * (1.0 - sigm))

def transpose_conv(cotangent, kernel):
    height, breadth, channels = cotangent.shape
    padded = jnp.pad(cotangent, ((1, 1), (1, 1), (0, 0)))
    summed = jnp.zeros((height * breadth, channels), jnp.float32)
    for tap_row in range(3):
        for tap_col in range(3):
            window = padded[2 - tap_row:2 - tap_row + height, 2 - tap_col:2 - tap_col + breadth].reshape(-1, channels)
            summed = summed + jnp.dot(window, kernel[tap_row, tap_col].T, preferred_element_type=jnp.float32)
    return summed.reshape(height, breadth, channels)

def weight_grad(activation, cotangent):
    height, breadth, channels = cotangent.shape
    padded = jnp.pad(activation, ((1, 1), (1, 1), (0, 0)))
    flat_grad = cotangent.reshape(-1, channels)
    taps = []
    for tap_row in range(3):
        for tap_col in range(3):
            window = padded[tap_row:tap_row + height, tap_col:tap_col + breadth].reshape(-1, channels)
            taps.append(lax.dot_general(window, flat_grad, (((0,), (0,)), ((), ())), preferred_element_type=jnp.float32))
    return jnp.stack(taps).reshape(3, 3, channels, channels)

def reference(grad_out, dec_pre, ctrl_out, ctrl_mid, ctrl_in, dec_weight, zero_weight, ctrl_weight):
    height, breadth, channels = grad_out.shape
    dec_grad = (silu_slope(dec_pre.astype(jnp.float32)) * transpose_conv(grad_out, dec_weight)).astype(jnp.bfloat16)
    flat_dec = dec_grad.reshape(-1, channels)
    grad_zero = lax.dot_general(ctrl_out.reshape(-1, channels), flat_dec, (((0,), (0,)), ((), ())), preferred_element_type=jnp.float32)
    ctrl_grad = jnp.dot(flat_dec, zero_weight.T, preferred_element_type=jnp.float32).astype(jnp.bfloat16).reshape(height, breadth, channels)
    mid_grad = (silu_slope(ctrl_mid.astype(jnp.float32)) * transpose_conv(ctrl_grad, ctrl_weight)).astype(jnp.bfloat16)
    act_mid = jax.nn.silu(ctrl_mid.astype(jnp.float32)).astype(jnp.bfloat16)
    act_in = jax.nn.silu(ctrl_in.astype(jnp.float32)).astype(jnp.bfloat16)
    grad_ctrl = weight_grad(act_mid, ctrl_grad)
    grad_in = weight_grad(act_in, mid_grad)
    return (grad_zero, grad_ctrl, grad_in)
```

```python
import functools

import jax
import jax.numpy as jnp
from jax import lax
from jax.experimental import pallas as pl
from jax.experimental.pallas import tpu as pltpu
from jax.sharding import PartitionSpec as P

BF16 = jnp.bfloat16
F32 = jnp.float32


def up(size, step):
    return -(-size // step) * step


def slope(values):
    sigm = jax.nn.sigmoid(values)
    return sigm * (1.0 + values * (1.0 - sigm))


def dot_nn(a, b):
    return lax.dot_general(a, b, (((1,), (0,)), ((), ())), preferred_element_type=F32)


def dot_nt(a, b):
    return lax.dot_general(a, b, (((1,), (1,)), ((), ())), preferred_element_type=F32)


class Plan:
    def __init__(self, height, width, channels, n_row, n_col):
        self.h, self.w, self.c = height, width, channels
        self.n_row, self.n_col = n_row, n_col
        self.cr, self.cc = channels // n_row, channels // n_col
        self.full = channels // 256 * 256
        self.rem = channels - self.full
        self.k1 = 3 * self.full + up(3 * self.rem, 256)
        wide = up(self.cc, 128)
        self.pq = wide if n_col * wide <= 2 * channels else self.cc
        self.np = n_col * self.pq
        self.qw = up(3 * self.cc, 128)
        self.rw = up(3 * self.cr, 128)
        self.hp = up(height + 2, 8)
        self.ring = 2 * width + 2 * self.hp
        self.px = height * width
        self.ls1 = 3 * self.qw + self.pq
        self.ls2 = 3 * self.rw


def spread(values, groups, size, pitch):
    rows = values.shape[0]
    pieces = []
    for g in range(groups):
        pieces.append(values[:, g * size : (g + 1) * size])
        if pitch > size:
            pieces.append(jnp.zeros((rows, pitch - size), values.dtype))
    return jnp.concatenate(pieces, axis=1)


def three_way(taps, starts, size, pitch):
    rows = taps[0].shape[0]
    pieces = []
    for s in starts:
        for t in taps:
            pieces.append(t[:, s : s + size])
        if pitch > 3 * size:
            pieces.append(jnp.zeros((rows, pitch - 3 * size), taps[0].dtype))
    return jnp.concatenate(pieces, axis=1)


def next_col(x, last):
    return jnp.concatenate([x[1:], last], axis=0)


def prev_col(x, first):
    return jnp.concatenate([first, x[:-1]], axis=0)


def prep_kernel(p, dw, cw, zw, mid, out, dec, w1, w2, zwp, out_t, act_t, slope_t, slope_dec):
    w1[...] = jnp.zeros_like(w1)
    zwp[...] = jnp.zeros_like(zwp)
    for a in range(3):
        for b in range(3):
            for q in range(p.n_col):
                rows = dw[3 * a + b, q * p.cc : (q + 1) * p.cc, :]
                at = q * p.pq
                base = a * p.k1
                w1[at : at + p.cc, base + b * p.full : base + (b + 1) * p.full] = rows[:, : p.full]
                if p.rem:
                    lane = base + 3 * p.full + b * p.rem
                    w1[at : at + p.cc, lane : lane + p.rem] = rows[:, p.full :]
    wide = p.n_col * p.qw
    for a in range(3):
        taps = [cw[3 * a + b] for b in range(3)]
        w2[:, a * wide : (a + 1) * wide] = three_way(
            taps, [q * p.cc for q in range(p.n_col)], p.cc, p.qw
        )
    for q in range(p.n_col):
        zwp[q * p.pq : q * p.pq + p.cc, :] = spread(
            zw[q * p.cc : (q + 1) * p.cc, :], p.n_col, p.cc, p.pq
        )
    step = 128

    def block(i, carry):
        at = pl.multiple_of(i * step, step)
        v = mid[pl.ds(at, step), :].astype(F32)
        s = jax.nn.sigmoid(v)
        act_t[:, pl.ds(at, step)] = (v * s).T.astype(BF16)
        slope_t[:, pl.ds(at, step)] = (s * (1.0 + v * (1.0 - s))).T
        out_t[:, pl.ds(at, step)] = out[pl.ds(at, step), :].astype(F32).T.astype(BF16)
        slope_dec[pl.ds(at, step), :] = spread(
            slope(dec[pl.ds(at, step), :].astype(F32)), p.n_col, p.cc, p.pq
        )
        return carry

    lax.fori_loop(0, p.px // step, block, 0)


def prep(p, dw, cw, zw, mid, out, dec):
    shape = jax.ShapeDtypeStruct
    return pl.pallas_call(
        functools.partial(prep_kernel, p),
        out_shape=(
            shape((p.np, 3 * p.k1), BF16),
            shape((p.c, 3 * p.n_col * p.qw), BF16),
            shape((p.np, p.np), BF16),
            shape((p.c, p.px), BF16),
            shape((p.c, p.px), BF16),
            shape((p.c, p.px), F32),
            shape((p.px, p.np), F32),
        ),
        cost_estimate=pl.CostEstimate(
            flops=2_000_000_000, bytes_accessed=20_000_000, transcendentals=3 * p.px * p.c
        ),
        name="prep",
    )(dw, cw, zw, mid, out, dec)


def act_kernel(p, x_ref, top, bottom, left, right, a_in, edge):
    edge[0, : p.h + 2, :] = left[3, : p.h + 2, :].astype(F32)
    edge[1, : p.h + 2, :] = right[3, : p.h + 2, :].astype(F32)

    def put(r, x):
        x = x.astype(F32)
        taps = (prev_col(x, edge[0, pl.ds(r, 1), :]), x, next_col(x, edge[1, pl.ds(r, 1), :]))
        taps = [(t * jax.nn.sigmoid(t)).astype(BF16) for t in taps]
        at = pl.multiple_of(r * p.w, p.w)
        a_in[pl.ds(at, p.w), :] = three_way(
            taps, [g * p.cr for g in range(p.n_row)], p.cr, p.rw
        )

    put(0, top[3])
    put(p.h + 1, bottom[3])

    def body(i, carry):
        put(i + 1, x_ref[i])
        return carry

    lax.fori_loop(0, p.h, body, 0)


def act_columns(p, ctrl_in, top, bottom, left, right):
    return pl.pallas_call(
        functools.partial(act_kernel, p),
        out_shape=jax.ShapeDtypeStruct(((p.h + 2) * p.w, p.n_row * p.rw), BF16),
        scratch_shapes=[pltpu.VMEM((2, up(p.h + 2, 8), p.c), F32)],
        cost_estimate=pl.CostEstimate(
            flops=1_000_000_000, bytes_accessed=4_000_000, transcendentals=3 * p.px * p.c
        ),
        name="act_columns",
    )(ctrl_in, top, bottom, left, right)


def store_slots(p, source, keep, send):
    mine = lax.axis_index("row")
    label = lax.axis_index("col")
    label = label ^ (label >> 1)
    for rr in range(p.n_row):
        r = rr ^ mine
        target = send if rr & 1 else keep
        for qq in range(p.n_col):
            q = qq ^ label
            shift = 1
            gray = q
            while (1 << shift) <= p.n_col:
                gray = gray ^ (q >> shift)
                shift += 1
            target[rr >> 1, qq] = source(r, gray).astype(BF16)


def first_kernel(
    p, go, top, bottom, left, right, own_l, own_r, w1, zwp, out_t, act_t, slope_dec,
    g2, keep, send, g1, ring_in, strips, dec, dec_ring, cg, cg_ring, grads,
):
    rows = p.h + 4
    strips[...] = jnp.zeros_like(strips)
    for k, s in enumerate((own_l[0], left[1], left[0], right[1], right[0], own_r[1])):
        strips[k, :rows, :] = s.astype(F32)

    def lanes(taps):
        pieces = [t[:, : p.full] for t in taps]
        if p.rem:
            pieces += [t[:, p.full :] for t in taps]
        pad = p.k1 - 3 * p.c
        if pad:
            pieces.append(jnp.zeros((taps[0].shape[0], pad), BF16))
        return jnp.concatenate(pieces, axis=1)

    def put(i, x):
        x = x.astype(F32)
        taps = (next_col(x, strips[4, pl.ds(i, 1), :]), x, prev_col(x, strips[1, pl.ds(i, 1), :]))
        at = pl.multiple_of(i * p.w, p.w)
        g1[pl.ds(at, p.w), :] = lanes([t.astype(BF16) for t in taps])

    for k in range(2):
        put(k, top[k])
        put(p.h + 2 + k, bottom[k])

    def body(i, carry):
        put(i + 2, go[i])
        return carry

    lax.fori_loop(0, p.h, body, 0)

    w, hp = p.w, p.hp
    for a in range(3):
        ls = slice(a * p.k1, (a + 1) * p.k1)
        ring_in[:w, ls] = g1[(2 - a) * w : (3 - a) * w, :]
        ring_in[w : 2 * w, ls] = g1[(p.h + 3 - a) * w : (p.h + 4 - a) * w, :]
        for side in range(2):
            taps = [strips[3 * side + b, 2 - a : 2 - a + hp, :].astype(BF16) for b in range(3)]
            ring_in[2 * w + side * hp : 2 * w + (side + 1) * hp, ls] = lanes(taps)

    weights = w1[...]
    step = 256
    for m in range(p.px // step):
        at = m * step
        lhs = jnp.concatenate(
            [g1[(3 - a) * w + at : (3 - a) * w + at + step, :] for a in range(3)], axis=1
        )
        dec[at : at + step, :] = (
            dot_nt(lhs, weights) * slope_dec[at : at + step, :]
        ).astype(BF16)

    row, col = lax.axis_index("row"), lax.axis_index("col")
    has_top = (row > 0).astype(F32)
    has_bottom = (row < p.n_row - 1).astype(F32)
    has_left = (col > 0).astype(F32)
    has_right = (col < p.n_col - 1).astype(F32)
    line = lax.broadcasted_iota(jnp.int32, (hp, p.np), 0)
    corner = jnp.where(line == 0, has_top, jnp.where(line == p.h + 1, has_bottom, 1.0))
    sections = (
        (top[2], 0, w, has_top),
        (bottom[2], w, w, has_bottom),
        (left[2], 2 * w, hp, corner * has_left),
        (right[2], 2 * w + hp, hp, corner * has_right),
    )
    ring_back = dot_nt(ring_in[...], weights)
    for pre, at, size, mask in sections:
        pre = pre.astype(F32)
        if pre.shape[0] < size:
            pre = jnp.concatenate([pre, jnp.zeros((size - pre.shape[0], p.c), F32)], axis=0)
        factor = spread(slope(pre[:size]), p.n_col, p.cc, p.pq) * mask
        dec_ring[at : at + size, :] = (ring_back[at : at + size] * factor).astype(BF16)

    zero = dot_nn(out_t[...], dec[...])
    for q in range(p.n_col):
        for r in range(p.n_row):
            grads[q, r, : p.cr, 3 * p.qw :] = zero[
                r * p.cr : (r + 1) * p.cr, q * p.pq : (q + 1) * p.pq
            ]
    for m in range(p.px // step):
        cg[m * step : (m + 1) * step, :] = dot_nt(dec[m * step : (m + 1) * step, :], zwp[...])
    cg_ring[...] = dot_nt(dec_ring[...], zwp[...])

    def put2(r, x):
        taps = (
            next_col(x, cg_ring[pl.ds(2 * w + hp + r, 1), :]),
            x,
            prev_col(x, cg_ring[pl.ds(2 * w + r, 1), :]),
        )
        at = pl.multiple_of(r * w, w)
        g2[pl.ds(at, w), :] = three_way(
            [t.astype(BF16) for t in taps], [q * p.pq for q in range(p.n_col)], p.cc, p.qw
        )

    put2(0, cg_ring[:w, :])
    put2(p.h + 1, cg_ring[w : 2 * w, :])

    def body2(i, carry):
        put2(i + 1, cg[pl.ds(pl.multiple_of(i * w, w), w), :])
        return carry

    lax.fori_loop(0, p.h, body2, 0)

    for a in range(3):
        for q in range(p.n_col):
            tap = dot_nn(
                act_t[...], g2[(2 - a) * w : (2 - a) * w + p.px, q * p.qw : (q + 1) * p.qw]
            )
            for r in range(p.n_row):
                grads[q, r, : p.cr, a * p.qw : (a + 1) * p.qw] = tap[r * p.cr : (r + 1) * p.cr]
    store_slots(p, lambda r, q: grads[q, r, : p.cr, :], keep, send)


def first(p, go, top, bottom, left, right, own_l, own_r, w1, zwp, out_t, act_t, slope_dec):
    shape = jax.ShapeDtypeStruct
    slots = shape((p.n_row // 2, p.n_col, p.cr, p.ls1), BF16)
    return pl.pallas_call(
        functools.partial(first_kernel, p),
        out_shape=(shape(((p.h + 2) * p.w, p.n_col * p.qw), BF16), slots, slots),
        scratch_shapes=[
            pltpu.VMEM(((p.h + 4) * p.w, p.k1), BF16),
            pltpu.VMEM((p.ring, 3 * p.k1), BF16),
            pltpu.VMEM((6, up(p.hp + 2, 8), p.c), F32),
            pltpu.VMEM((p.px, p.np), BF16),
            pltpu.VMEM((p.ring, p.np), BF16),
            pltpu.VMEM((p.px, p.np), F32),
            pltpu.VMEM((p.ring, p.np), F32),
            pltpu.VMEM((p.n_col, p.n_row, up(p.cr, 8), p.ls1), F32),
        ],
        cost_estimate=pl.CostEstimate(
            flops=10_000_000_000, bytes_accessed=20_000_000, transcendentals=0
        ),
        name="first",
    )(go, top, bottom, left, right, own_l, own_r, w1, zwp, out_t, act_t, slope_dec)


def second_kernel(p, g2, a_in, w2, slope_t, keep, send, mid, grads):
    w = p.w
    step = 256
    for m in range(p.px // step):
        at = m * step
        rhs = jnp.concatenate(
            [g2[(2 - a) * w + at : (2 - a) * w + at + step, :] for a in range(3)], axis=1
        )
        mid[:, at : at + step] = (
            dot_nt(w2[...], rhs) * slope_t[:, at : at + step]
        ).astype(BF16)
    for a in range(3):
        for r in range(p.n_row):
            tap = dot_nn(mid[...], a_in[a * w : a * w + p.px, r * p.rw : (r + 1) * p.rw])
            for q in range(p.n_col):
                grads[r, q, : p.cc, a * p.rw : (a + 1) * p.rw] = tap[q * p.cc : (q + 1) * p.cc]
    store_slots(p, lambda r, q: grads[r, q, : p.cc, :], keep, send)


def second(p, g2, a_in, w2, slope_t):
    slots = jax.ShapeDtypeStruct((p.n_row // 2, p.n_col, p.cc, p.ls2), BF16)
    return pl.pallas_call(
        functools.partial(second_kernel, p),
        out_shape=(slots, slots),
        scratch_shapes=[
            pltpu.VMEM((p.c, p.px), BF16),
            pltpu.VMEM((p.n_row, p.n_col, up(p.cc, 8), p.ls2), F32),
        ],
        cost_estimate=pl.CostEstimate(
            flops=6_000_000_000, bytes_accessed=10_000_000, transcendentals=0
        ),
        name="second",
    )(g2, a_in, w2, slope_t)


def gray(i):
    return i ^ (i >> 1)


def swap(values, axis, bit):
    count = lax.axis_size(axis)
    if axis == "row":
        pairs = [(i, i ^ (1 << bit)) for i in range(count)]
    else:
        place = {gray(i): i for i in range(count)}
        pairs = [(i, place[gray(i) ^ (1 << bit)]) for i in range(count)]
    return lax.ppermute(values, axis, pairs)


def total(pieces):
    summed = pieces[0].astype(F32)
    for piece in pieces[1:]:
        summed = summed + piece.astype(F32)
    return summed


class Chain:
    def __init__(self, pieces, order):
        self.pieces, self.order = pieces, list(order)
        self.dims = sorted(order)

    def step(self):
        dim = self.order.pop(0)
        at = self.dims.index(dim)
        self.dims.pop(at)
        rank = self.pieces[0].ndim
        other = tuple([slice(None)] * at + [1])
        own = tuple([slice(None)] * at + [0])
        sent = total([x[other] for x in self.pieces]).astype(BF16)
        axis, bit = dim[1], dim[2]
        self.pieces = [x[own] for x in self.pieces] + [swap(sent, axis, bit)]


def dims_of(p):
    k_row = p.n_row.bit_length() - 1
    k_col = p.n_col.bit_length() - 1
    row = [(i, "row", k_row - 1 - i) for i in range(k_row - 1)]
    col = [(len(row) + i, "col", k_col - 1 - i) for i in range(k_col)]
    return row, col


def as_cube(p, values):
    row, col = dims_of(p)
    return values.reshape((2,) * (len(row) + len(col)) + values.shape[2:])


def last_kernel(p, n1, *refs):
    gz, gc, gi = refs[-3:]
    one = jnp.concatenate([x[...] for x in refs[:n1]], axis=1)
    gz[...] = one[:, 3 * p.qw : 3 * p.qw + p.cc]
    for a in range(3):
        for b in range(3):
            at = a * p.qw + b * p.cc
            gc[a, b] = one[:, at : at + p.cc]
    two = jnp.concatenate([x[...] for x in refs[n1:-3]], axis=0).T
    for a in range(3):
        for b in range(3):
            at = a * p.rw + b * p.cr
            gi[a, b] = two[at : at + p.cr, :]


def last(p, chains1, chains2):
    shape = jax.ShapeDtypeStruct
    return pl.pallas_call(
        functools.partial(last_kernel, p, len(chains1)),
        out_shape=(
            shape((p.cr, p.cc), F32),
            shape((3, 3, p.cr, p.cc), F32),
            shape((3, 3, p.cr, p.cc), F32),
        ),
        name="last",
    )(*[total(c.pieces) for c in chains1 + chains2])


def halos(p, go, dec_pre, ctrl_in):
    count = lax.axis_size("row")
    down = [(i, i + 1) for i in range(count - 1)]
    upward = [(i + 1, i) for i in range(count - 1)]
    top = lax.ppermute(
        jnp.concatenate([go[-2:], dec_pre[-1:], ctrl_in[-1:]], axis=0), "row", down
    )
    bottom = lax.ppermute(
        jnp.concatenate([go[:2], dec_pre[:1], ctrl_in[:1]], axis=0), "row", upward
    )
    grad = jnp.concatenate([top[:2], go, bottom[:2]], axis=0)
    spare = jnp.zeros((2, 1, p.c), BF16)

    def strip(g0, g1, edge):
        return jnp.stack(
            [
                grad[:, g0],
                grad[:, g1],
                jnp.concatenate([top[2:3, edge], dec_pre[:, edge], bottom[2:3, edge], spare[:, 0]]),
                jnp.concatenate([top[3:4, edge], ctrl_in[:, edge], bottom[3:4, edge], spare[:, 0]]),
            ]
        )

    own_l = strip(0, 1, 0)
    own_r = strip(p.w - 2, p.w - 1, p.w - 1)
    count = lax.axis_size("col")
    forward = [(i, i + 1) for i in range(count - 1)]
    backward = [(i + 1, i) for i in range(count - 1)]
    left = lax.ppermute(own_r, "col", forward)
    right = lax.ppermute(own_l, "col", backward)
    return top, bottom, left, right, own_l, own_r


def on_device(grad_out, dec_pre, ctrl_out, ctrl_mid, ctrl_in, dec_weight, zero_weight, ctrl_weight):
    height, width, channels = grad_out.shape
    p = Plan(height, width, channels, lax.axis_size("row"), lax.axis_size("col"))
    flat = (p.px, p.c)
    taps = (9, p.c, p.c)
    w1, w2, zwp, out_t, act_t, slope_t, slope_dec = prep(
        p,
        dec_weight.reshape(taps),
        ctrl_weight.reshape(taps),
        zero_weight,
        ctrl_mid.reshape(flat),
        ctrl_out.reshape(flat),
        dec_pre.reshape(flat),
    )
    top, bottom, left, right, own_l, own_r = halos(p, grad_out, dec_pre, ctrl_in)
    g2, keep1, send1 = first(
        p, grad_out, top, bottom, left, right, own_l, own_r, w1, zwp, out_t, act_t, slope_dec
    )
    row, col = dims_of(p)
    got1 = swap(send1, "row", 0)
    a_in = act_columns(p, ctrl_in, top, bottom, left, right)
    keep2, send2 = second(p, g2, a_in, w2, slope_t)
    chains1 = [Chain([as_cube(p, keep1), as_cube(p, got1)], row[::-1] + col)]
    chains1[0].step()
    got2 = swap(send2, "row", 0)
    cubes = [as_cube(p, keep2), as_cube(p, got2)]
    half = p.cc // 2 if (p.cc // 2) % 8 == 0 else p.cc
    parts = [(0, half), (half, p.cc)] if half < p.cc else [(0, p.cc)]
    orders = [col + row, col[::-1] + row[::-1]]
    chains2 = [
        Chain([x[..., lo:hi, :] for x in cubes], order) for (lo, hi), order in zip(parts, orders)
    ]
    live = chains1 + chains2
    while any(c.order for c in live):
        for c in live:
            if c.order:
                c.step()
    return last(p, chains1, chains2)


def solution(mesh):
    in_specs = (
        P("row", "col", None),
        P("row", "col", None),
        P("row", "col", None),
        P("row", "col", None),
        P("row", "col", None),
        P(),
        P(),
        P(),
    )
    out_specs = (P("row", "col"), P(None, None, "row", "col"), P(None, None, "row", "col"))
    return jax.shard_map(
        on_device, mesh=mesh, in_specs=in_specs, out_specs=out_specs, check_vma=False
    )
```

```python
import functools

import jax
import jax.numpy as jnp
from jax import lax
from jax.experimental import pallas as pl
from jax.experimental.pallas import tpu as pltpu
from jax.sharding import PartitionSpec as P

BF16 = jnp.bfloat16
F32 = jnp.float32


def up(size, step):
    return -(-size // step) * step


def vm(shape, dtype):
    return pltpu.VMEM(shape, dtype)


def near(*arrays):
    return [pltpu.with_memory_space_constraint(x, pltpu.VMEM) for x in arrays]


def slope(values):
    sigm = jax.nn.sigmoid(values)
    return sigm * (1.0 + values * (1.0 - sigm))


def dot_nn(a, b):
    return lax.dot_general(a, b, (((1,), (0,)), ((), ())), preferred_element_type=F32)


def dot_nt(a, b):
    return lax.dot_general(a, b, (((1,), (1,)), ((), ())), preferred_element_type=F32)


class Plan:
    def __init__(self, height, width, channels, n_row, n_col):
        self.h, self.w, self.c = height, width, channels
        self.n_row, self.n_col = n_row, n_col
        self.cr, self.cc = channels // n_row, channels // n_col
        self.full = channels // 256 * 256
        self.rem = channels - self.full
        self.k1 = 3 * self.full + up(3 * self.rem, 256)
        wide = up(self.cc, 128)
        self.pq = wide if n_col * wide <= 2 * channels else self.cc
        self.np = n_col * self.pq
        self.qw = up(3 * self.cc, 128)
        self.rw = up(3 * self.cr, 128)
        self.hp = up(height + 2, 8)
        self.ring = 2 * width + 2 * self.hp
        self.px = height * width
        self.ls1 = 3 * self.qw + self.pq
        self.ls2 = 3 * self.rw


def spread(values, groups, size, pitch):
    rows = values.shape[0]
    pieces = []
    for g in range(groups):
        pieces.append(values[:, g * size : (g + 1) * size])
        if pitch > size:
            pieces.append(jnp.zeros((rows, pitch - size), values.dtype))
    return jnp.concatenate(pieces, axis=1)


def three_way(taps, starts, size, pitch):
    rows = taps[0].shape[0]
    pieces = []
    for s in starts:
        for t in taps:
            pieces.append(t[:, s : s + size])
        if pitch > 3 * size:
            pieces.append(jnp.zeros((rows, pitch - 3 * size), taps[0].dtype))
    return jnp.concatenate(pieces, axis=1)


def next_col(x, last):
    return jnp.concatenate([x[1:], last], axis=0)


def prev_col(x, first):
    return jnp.concatenate([first, x[:-1]], axis=0)


def prep_kernel(p, dw, cw, zw, mid, out, dec, w1, w2, zwp, out_t, act_t, slope_t, slope_dec):
    w1[...] = jnp.zeros_like(w1)
    zwp[...] = jnp.zeros_like(zwp)
    for a in range(3):
        for b in range(3):
            for q in range(p.n_col):
                rows = dw[3 * a + b, q * p.cc : (q + 1) * p.cc, :]
                at = q * p.pq
                base = a * p.k1
                w1[at : at + p.cc, base + b * p.full : base + (b + 1) * p.full] = rows[:, : p.full]
                if p.rem:
                    lane = base + 3 * p.full + b * p.rem
                    w1[at : at + p.cc, lane : lane + p.rem] = rows[:, p.full :]
    wide = p.n_col * p.qw
    for a in range(3):
        taps = [cw[3 * a + b] for b in range(3)]
        w2[:, a * wide : (a + 1) * wide] = three_way(
            taps, [q * p.cc for q in range(p.n_col)], p.cc, p.qw
        )
    for q in range(p.n_col):
        zwp[q * p.pq : q * p.pq + p.cc, :] = spread(
            zw[q * p.cc : (q + 1) * p.cc, :], p.n_col, p.cc, p.pq
        )
    step = 128

    def block(i, carry):
        at = pl.multiple_of(i * step, step)
        v = mid[pl.ds(at, step), :].astype(F32)
        s = jax.nn.sigmoid(v)
        act_t[:, pl.ds(at, step)] = (v * s).T.astype(BF16)
        slope_t[:, pl.ds(at, step)] = (s * (1.0 + v * (1.0 - s))).T
        out_t[:, pl.ds(at, step)] = out[pl.ds(at, step), :].astype(F32).T.astype(BF16)
        slope_dec[pl.ds(at, step), :] = spread(
            slope(dec[pl.ds(at, step), :].astype(F32)), p.n_col, p.cc, p.pq
        )
        return carry

    lax.fori_loop(0, p.px // step, block, 0, unroll=2)


def prep(p, dw, cw, zw, mid, out, dec):
    return pl.pallas_call(
        functools.partial(prep_kernel, p),
        out_shape=(
            vm((p.np, 3 * p.k1), BF16),
            vm((p.c, 3 * p.n_col * p.qw), BF16),
            vm((p.np, p.np), BF16),
            vm((p.c, p.px), BF16),
            vm((p.c, p.px), BF16),
            vm((p.c, p.px), F32),
            vm((p.px, p.np), F32),
        ),
        cost_estimate=pl.CostEstimate(
            flops=2_000_000_000, bytes_accessed=20_000_000, transcendentals=3 * p.px * p.c
        ),
        compiler_params=pltpu.CompilerParams(vmem_limit_bytes=20 << 20),
        name="prep",
    )(dw, cw, zw, mid, out, dec)


def act_kernel(p, x_ref, top, bottom, left, right, a_in, edge):
    edge[0, : p.h + 2, :] = left[3, : p.h + 2, :].astype(F32)
    edge[1, : p.h + 2, :] = right[3, : p.h + 2, :].astype(F32)

    def put(r, x):
        x = x.astype(F32)
        taps = (prev_col(x, edge[0, pl.ds(r, 1), :]), x, next_col(x, edge[1, pl.ds(r, 1), :]))
        taps = [(t * jax.nn.sigmoid(t)).astype(BF16) for t in taps]
        at = pl.multiple_of(r * p.w, p.w)
        a_in[pl.ds(at, p.w), :] = three_way(
            taps, [g * p.cr for g in range(p.n_row)], p.cr, p.rw
        )

    put(0, top[3])
    put(p.h + 1, bottom[3])

    def body(i, carry):
        put(i + 1, x_ref[i])
        return carry

    lax.fori_loop(0, p.h, body, 0, unroll=8)


def act_columns(p, ctrl_in, top, bottom, left, right):
    return pl.pallas_call(
        functools.partial(act_kernel, p),
        out_shape=vm(((p.h + 2) * p.w, p.n_row * p.rw), BF16),
        scratch_shapes=[pltpu.VMEM((2, up(p.h + 2, 8), p.c), F32)],
        cost_estimate=pl.CostEstimate(
            flops=1_000_000_000, bytes_accessed=4_000_000, transcendentals=3 * p.px * p.c
        ),
        compiler_params=pltpu.CompilerParams(vmem_limit_bytes=8 << 20),
        name="act_columns",
    )(ctrl_in, top, bottom, left, right)


def store_slots(p, source, keep, send):
    mine = lax.axis_index("row")
    label = lax.axis_index("col")
    label = label ^ (label >> 1)
    for rr in range(p.n_row):
        r = rr ^ mine
        target = send if rr & 1 else keep
        for qq in range(p.n_col):
            q = qq ^ label
            shift = 1
            gray = q
            while (1 << shift) <= p.n_col:
                gray = gray ^ (q >> shift)
                shift += 1
            target[(rr >> 1) * p.n_col + qq] = source(r, gray).astype(BF16)


def first_kernel(
    p, go, top, bottom, left, right, own_l, own_r, w1, zwp, out_t, act_t, slope_dec,
    g2, keep, send, g1, ring_in, strips, dec, dec_ring, cg, cg_ring, grads,
):
    rows = p.h + 4
    strips[...] = jnp.zeros_like(strips)
    for k, s in enumerate((own_l[0], left[1], left[0], right[1], right[0], own_r[1])):
        strips[k, :rows, :] = s.astype(F32)

    def lanes(taps):
        pieces = [t[:, : p.full] for t in taps]
        if p.rem:
            pieces += [t[:, p.full :] for t in taps]
        pad = p.k1 - 3 * p.c
        if pad:
            pieces.append(jnp.zeros((taps[0].shape[0], pad), BF16))
        return jnp.concatenate(pieces, axis=1)

    def put(i, x):
        x = x.astype(F32)
        taps = (next_col(x, strips[4, pl.ds(i, 1), :]), x, prev_col(x, strips[1, pl.ds(i, 1), :]))
        at = pl.multiple_of(i * p.w, p.w)
        g1[pl.ds(at, p.w), :] = lanes([t.astype(BF16) for t in taps])

    for k in range(2):
        put(k, top[k])
        put(p.h + 2 + k, bottom[k])

    def body(i, carry):
        put(i + 2, go[i])
        return carry

    lax.fori_loop(0, p.h, body, 0, unroll=8)

    w, hp = p.w, p.hp
    for a in range(3):
        ls = slice(a * p.k1, (a + 1) * p.k1)
        ring_in[:w, ls] = g1[(2 - a) * w : (3 - a) * w, :]
        ring_in[w : 2 * w, ls] = g1[(p.h + 3 - a) * w : (p.h + 4 - a) * w, :]
        for side in range(2):
            taps = [strips[3 * side + b, 2 - a : 2 - a + hp, :].astype(BF16) for b in range(3)]
            ring_in[2 * w + side * hp : 2 * w + (side + 1) * hp, ls] = lanes(taps)

    weights = w1[...]
    step = 256
    for m in range(p.px // step):
        at = m * step
        lhs = jnp.concatenate(
            [g1[(3 - a) * w + at : (3 - a) * w + at + step, :] for a in range(3)], axis=1
        )
        dec[at : at + step, :] = (
            dot_nt(lhs, weights) * slope_dec[at : at + step, :]
        ).astype(BF16)

    row, col = lax.axis_index("row"), lax.axis_index("col")
    has_top = (row > 0).astype(F32)
    has_bottom = (row < p.n_row - 1).astype(F32)
    has_left = (col > 0).astype(F32)
    has_right = (col < p.n_col - 1).astype(F32)
    line = lax.broadcasted_iota(jnp.int32, (hp, p.np), 0)
    corner = jnp.where(line == 0, has_top, jnp.where(line == p.h + 1, has_bottom, 1.0))
    sections = (
        (top[2], 0, w, has_top),
        (bottom[2], w, w, has_bottom),
        (left[2], 2 * w, hp, corner * has_left),
        (right[2], 2 * w + hp, hp, corner * has_right),
    )
    ring_back = dot_nt(ring_in[...], weights)
    for pre, at, size, mask in sections:
        pre = pre.astype(F32)
        if pre.shape[0] < size:
            pre = jnp.concatenate([pre, jnp.zeros((size - pre.shape[0], p.c), F32)], axis=0)
        factor = spread(slope(pre[:size]), p.n_col, p.cc, p.pq) * mask
        dec_ring[at : at + size, :] = (ring_back[at : at + size] * factor).astype(BF16)

    zero = dot_nn(out_t[...], dec[...])
    for q in range(p.n_col):
        for r in range(p.n_row):
            grads[q, r, : p.cr, 3 * p.qw :] = zero[
                r * p.cr : (r + 1) * p.cr, q * p.pq : (q + 1) * p.pq
            ]
    for m in range(p.px // step):
        cg[m * step : (m + 1) * step, :] = dot_nt(dec[m * step : (m + 1) * step, :], zwp[...])
    cg_ring[...] = dot_nt(dec_ring[...], zwp[...])

    def put2(r, x):
        taps = (
            next_col(x, cg_ring[pl.ds(2 * w + hp + r, 1), :]),
            x,
            prev_col(x, cg_ring[pl.ds(2 * w + r, 1), :]),
        )
        at = pl.multiple_of(r * w, w)
        g2[pl.ds(at, w), :] = three_way(
            [t.astype(BF16) for t in taps], [q * p.pq for q in range(p.n_col)], p.cc, p.qw
        )

    put2(0, cg_ring[:w, :])
    put2(p.h + 1, cg_ring[w : 2 * w, :])

    def body2(i, carry):
        put2(i + 1, cg[pl.ds(pl.multiple_of(i * w, w), w), :])
        return carry

    lax.fori_loop(0, p.h, body2, 0, unroll=8)

    for a in range(3):
        for q in range(p.n_col):
            tap = dot_nn(
                act_t[...], g2[(2 - a) * w : (2 - a) * w + p.px, q * p.qw : (q + 1) * p.qw]
            )
            for r in range(p.n_row):
                grads[q, r, : p.cr, a * p.qw : (a + 1) * p.qw] = tap[r * p.cr : (r + 1) * p.cr]
    store_slots(p, lambda r, q: grads[q, r, : p.cr, :], keep, send)


def first(p, go, top, bottom, left, right, own_l, own_r, w1, zwp, out_t, act_t, slope_dec):
    shape = jax.ShapeDtypeStruct
    slots = vm((p.n_row // 2 * p.n_col, p.cr, p.ls1), BF16)
    return pl.pallas_call(
        functools.partial(first_kernel, p),
        out_shape=(vm(((p.h + 2) * p.w, p.n_col * p.qw), BF16), slots, slots),
        scratch_shapes=[
            pltpu.VMEM(((p.h + 4) * p.w, p.k1), BF16),
            pltpu.VMEM((p.ring, 3 * p.k1), BF16),
            pltpu.VMEM((6, up(p.hp + 2, 8), p.c), F32),
            pltpu.VMEM((p.px, p.np), BF16),
            pltpu.VMEM((p.ring, p.np), BF16),
            pltpu.VMEM((p.px, p.np), F32),
            pltpu.VMEM((p.ring, p.np), F32),
            pltpu.VMEM((p.n_col, p.n_row, up(p.cr, 8), p.ls1), F32),
        ],
        cost_estimate=pl.CostEstimate(
            flops=10_000_000_000, bytes_accessed=20_000_000, transcendentals=0
        ),
        compiler_params=pltpu.CompilerParams(vmem_limit_bytes=28 << 20),
        name="first",
    )(
        go, top, bottom, left, right, own_l, own_r,
        *near(w1, zwp, out_t, act_t, slope_dec),
    )


def second_kernel(p, g2, a_in, w2, slope_t, keep, send, mid, grads):
    w = p.w
    step = 256
    for m in range(p.px // step):
        at = m * step
        rhs = jnp.concatenate(
            [g2[(2 - a) * w + at : (2 - a) * w + at + step, :] for a in range(3)], axis=1
        )
        mid[:, at : at + step] = (
            dot_nt(w2[...], rhs) * slope_t[:, at : at + step]
        ).astype(BF16)
    for a in range(3):
        for r in range(p.n_row):
            tap = dot_nn(mid[...], a_in[a * w : a * w + p.px, r * p.rw : (r + 1) * p.rw])
            for q in range(p.n_col):
                grads[r, q, : p.cc, a * p.rw : (a + 1) * p.rw] = tap[q * p.cc : (q + 1) * p.cc]
    store_slots(p, lambda r, q: grads[r, q, : p.cc, :], keep, send)


def second(p, g2, a_in, w2, slope_t):
    slots = vm((p.n_row // 2 * p.n_col, p.cc, p.ls2), BF16)
    return pl.pallas_call(
        functools.partial(second_kernel, p),
        out_shape=(slots, slots),
        scratch_shapes=[
            pltpu.VMEM((p.c, p.px), BF16),
            pltpu.VMEM((p.n_row, p.n_col, up(p.cc, 8), p.ls2), F32),
        ],
        cost_estimate=pl.CostEstimate(
            flops=6_000_000_000, bytes_accessed=10_000_000, transcendentals=0
        ),
        compiler_params=pltpu.CompilerParams(vmem_limit_bytes=16 << 20),
        name="second",
    )(*near(g2, a_in, w2, slope_t))


def gray(i):
    return i ^ (i >> 1)


def swap(name, values, dim):
    axis, bit = dim
    count = lax.axis_size(axis)
    if axis == "row":
        pairs = [(i, i ^ (1 << bit)) for i in range(count)]
    else:
        place = {gray(i): i for i in range(count)}
        pairs = [(i, place[gray(i) ^ (1 << bit)]) for i in range(count)]
    with jax.named_scope(name):
        return lax.ppermute(values, axis, pairs)


class Part:
    def __init__(self, dims, rows, lanes, keep, got=None):
        self.dims, self.rows, self.lanes = dims, rows, lanes
        self.keep, self.got = keep, got


def slot_of(bits, dims):
    at = 0
    for dim in dims:
        at = 2 * at + bits[dim]
    return at


def assignments(dims):
    for code in range(1 << len(dims)):
        yield {dim: (code >> i) & 1 for i, dim in enumerate(dims)}


def overlap(a, b):
    lo, hi = max(a[0], b[0]), min(a[1], b[1])
    return (lo, hi) if lo < hi else None


def mix_kernel(sources, targets, *refs):
    ins = refs[: 2 * len(sources)]
    outs = refs[2 * len(sources) :]
    for k, source in enumerate(sources):
        keep, got = ins[2 * k], ins[2 * k + 1]
        for n, target in enumerate(targets):
            rows = overlap(source.rows, target.rows)
            lanes = overlap(source.lanes, target.lanes)
            if rows is None or lanes is None:
                continue
            sr = slice(rows[0] - source.rows[0], rows[1] - source.rows[0])
            sl = slice(lanes[0] - source.lanes[0], lanes[1] - source.lanes[0])
            tr = slice(rows[0] - target.rows[0], rows[1] - target.rows[0])
            tl = slice(lanes[0] - target.lanes[0], lanes[1] - target.lanes[0])
            for bits in assignments(source.dims):
                at = slot_of(bits, source.dims)
                value = keep[at, sr, sl].astype(F32) + got[at, sr, sl].astype(F32)
                goes = bits[target.dims[0]]
                out = outs[2 * n + goes]
                out[slot_of(bits, target.dims[1:]), tr, tl] = value.astype(out.dtype)


def mix(name, sources, targets):
    shapes = []
    for t in targets:
        shape = (1 << (len(t.dims) - 1), t.rows[1] - t.rows[0], t.lanes[1] - t.lanes[0])
        shapes += [vm(shape, F32), vm(shape, BF16)]
    size = sum(s.keep.size for s in sources)
    bare = [Part(s.dims, s.rows, s.lanes, None) for s in sources]
    with jax.named_scope(name):
        results = pl.pallas_call(
            functools.partial(mix_kernel, bare, targets),
            out_shape=tuple(shapes),
            compiler_params=pltpu.CompilerParams(vmem_limit_bytes=6 << 20),
            cost_estimate=pl.CostEstimate(
                flops=200_000_000, bytes_accessed=8 * size, transcendentals=0
            ),
            name=name,
        )(*near(*[x for s in sources for x in (s.keep, s.got)]))
    return [
        (Part(t.dims[1:], t.rows, t.lanes, results[2 * i]), results[2 * i + 1], t.dims[0])
        for i, t in enumerate(targets)
    ]


class Chain:
    def __init__(self, name, rows, lanes, cut, dims, early, late):
        self.name, self.rows, self.lanes, self.cut = name, rows, lanes, cut
        self.early, self.late = early, late
        self.whole = Part(dims, (0, rows), (0, lanes), None)
        self.parts = []

    def halves(self, order_a, order_b):
        if self.cut[0] == "rows":
            at = self.cut[1]
            return [
                Part(order_a, (0, at), (0, self.lanes), None),
                Part(order_b, (at, self.rows), (0, self.lanes), None),
            ]
        at = self.cut[1]
        return [
            Part(order_a, (0, self.rows), (0, at), None),
            Part(order_b, (0, self.rows), (at, self.lanes), None),
        ]

    def send(self, stage, mixed):
        self.parts = []
        for i, (part, sent, dim) in enumerate(mixed):
            part.got = swap(f"{self.name}{stage}{'ab'[i]}", sent, dim)
            self.parts.append(part)

    def begin(self, keep, got):
        self.whole.keep, self.whole.got = keep, got
        e, l = self.early, self.late
        self.send(1, mix(f"{self.name}mix1", [self.whole], self.halves(e + l, e[::-1] + l)))

    def second(self):
        mixed = []
        for i, part in enumerate(self.parts):
            target = Part(part.dims, part.rows, part.lanes, None)
            mixed += mix(f"{self.name}mix2{'ab'[i]}", [part], [target])
        self.send(2, mixed)

    def third(self):
        target = Part(self.late, (0, self.rows), (0, self.lanes), None)
        self.send(3, mix(f"{self.name}mix3", self.parts, [target]))

    def later(self, stage):
        part = self.parts[0]
        target = Part(part.dims, part.rows, part.lanes, None)
        self.send(stage, mix(f"{self.name}mix{stage}", [part], [target]))


def dims_of(p):
    k_row = p.n_row.bit_length() - 1
    k_col = p.n_col.bit_length() - 1
    row = [("row", i) for i in range(k_row - 1, 0, -1)]
    col = [("col", i) for i in range(k_col - 1, -1, -1)]
    return row, col


def last_kernel(p, keep1, got1, keep2, got2, gz, gc, gi):
    one = keep1[0] + got1[0].astype(F32)
    gz[...] = one[:, 3 * p.qw : 3 * p.qw + p.cc]
    for a in range(3):
        for b in range(3):
            at = a * p.qw + b * p.cc
            gc[a, b] = one[:, at : at + p.cc]
    two = (keep2[0] + got2[0].astype(F32)).T
    for a in range(3):
        for b in range(3):
            at = a * p.rw + b * p.cr
            gi[a, b] = two[at : at + p.cr, :]


def last(p, one, two):
    shape = jax.ShapeDtypeStruct
    return pl.pallas_call(
        functools.partial(last_kernel, p),
        out_shape=(
            shape((p.cr, p.cc), F32),
            shape((3, 3, p.cr, p.cc), F32),
            shape((3, 3, p.cr, p.cc), F32),
        ),
        compiler_params=pltpu.CompilerParams(vmem_limit_bytes=8 << 20),
        name="last",
    )(*near(one.keep, one.got, two.keep, two.got))


def halos(p, go, dec_pre, ctrl_in):
    count = lax.axis_size("row")
    down = [(i, i + 1) for i in range(count - 1)]
    upward = [(i + 1, i) for i in range(count - 1)]
    top = lax.ppermute(
        jnp.concatenate([go[-2:], dec_pre[-1:], ctrl_in[-1:]], axis=0), "row", down
    )
    bottom = lax.ppermute(
        jnp.concatenate([go[:2], dec_pre[:1], ctrl_in[:1]], axis=0), "row", upward
    )
    grad = jnp.concatenate([top[:2], go, bottom[:2]], axis=0)
    spare = jnp.zeros((2, 1, p.c), BF16)

    def strip(g0, g1, edge):
        return jnp.stack(
            [
                grad[:, g0],
                grad[:, g1],
                jnp.concatenate([top[2:3, edge], dec_pre[:, edge], bottom[2:3, edge], spare[:, 0]]),
                jnp.concatenate([top[3:4, edge], ctrl_in[:, edge], bottom[3:4, edge], spare[:, 0]]),
            ]
        )

    own_l = strip(0, 1, 0)
    own_r = strip(p.w - 2, p.w - 1, p.w - 1)
    count = lax.axis_size("col")
    forward = [(i, i + 1) for i in range(count - 1)]
    backward = [(i + 1, i) for i in range(count - 1)]
    left = lax.ppermute(own_r, "col", forward)
    right = lax.ppermute(own_l, "col", backward)
    return top, bottom, left, right, own_l, own_r


def on_device(grad_out, dec_pre, ctrl_out, ctrl_mid, ctrl_in, dec_weight, zero_weight, ctrl_weight):
    height, width, channels = grad_out.shape
    p = Plan(height, width, channels, lax.axis_size("row"), lax.axis_size("col"))
    flat = (p.px, p.c)
    taps = (9, p.c, p.c)
    w1, w2, zwp, out_t, act_t, slope_t, slope_dec = prep(
        p,
        dec_weight.reshape(taps),
        ctrl_weight.reshape(taps),
        zero_weight,
        ctrl_mid.reshape(flat),
        ctrl_out.reshape(flat),
        dec_pre.reshape(flat),
    )
    top, bottom, left, right, own_l, own_r = halos(p, grad_out, dec_pre, ctrl_in)
    g2, keep1, send1 = first(
        p, grad_out, top, bottom, left, right, own_l, own_r, w1, zwp, out_t, act_t, slope_dec
    )
    row, col = dims_of(p)
    core = ("row", 0)
    got1 = swap("onecore", send1, core)
    a_in = act_columns(p, ctrl_in, top, bottom, left, right)
    one = Chain("one", p.cr, p.ls1, ("lanes", up(p.ls1 // 2, 128)), row + col, row, col)
    one.begin(keep1, got1)
    keep2, send2 = second(p, g2, a_in, w2, slope_t)
    got2 = swap("twocore", send2, core)
    half = p.cc // 2
    cut = ("rows", half) if half % 8 == 0 else ("lanes", up(p.ls2 // 2, 128))
    two = Chain("two", p.cc, p.ls2, cut, row + col, col, row)
    two.begin(keep2, got2)
    for chain in (one, two):
        for stage in range(2, len(chain.early) + 1):
            chain.second()
        chain.third()
        for stage in range(4, len(chain.late) + 3):
            chain.later(stage)
    return last(p, one.parts[0], two.parts[0])


def solution(mesh):
    in_specs = (
        P("row", "col", None),
        P("row", "col", None),
        P("row", "col", None),
        P("row", "col", None),
        P("row", "col", None),
        P(),
        P(),
        P(),
    )
    out_specs = (P("row", "col"), P(None, None, "row", "col"), P(None, None, "row", "col"))
    return jax.shard_map(
        on_device, mesh=mesh, in_specs=in_specs, out_specs=out_specs, check_vma=False
    )
```
